128 devices in a mesh: grp: 8 (over z, y_lo), dev: 16 (over x, y_hi, core).
Axes of the slice: x: 4, y: 4 (y_hi: 2, y_lo: 2; y = y_hi * 2 + y_lo), z: 4, core: 2. Of those that a mesh axis runs over, the one named last changes fastest.
Arguments:
- vertex_values: bfloat16 [8192, 128, 256], P(('grp', 'dev')), may hold values from -6 to 6
- position_domain_label: int32 [8192], P(('grp', 'dev')), may hold values from 0 to 64, as said below
- position_vertex_tally: int32 [8192], P(('grp', 'dev')), may hold values from 0 to 128, as said below
- normalizer_gain: float32 [256], replicated, may hold values from 0.1 to 1.9
- embedding_matrix: bfloat16 [256, 256], replicated, may hold values from -0.375 to 0.375
- partition_input_matrix: bfloat16 [256, 256], replicated, may hold values from -0.375 to 0.375
- partition_score_matrix: bfloat16 [32, 64], replicated, may hold values from -60 to 60
- softmax_sharpness: float32 [8], replicated, may hold values from 0.3 to 1
- partition_attention_maps: float32 [3, 32, 32], replicated, may hold values from -10 to 10
- readout_matrix: bfloat16 [256, 256], replicated, may hold values from -1.5 to 1.5
Outputs:
- updated: bfloat16 [8192, 128, 256], P(('grp', 'dev'))
The draws below stay inside these ranges and needn't reach their ends.
Inputs may be any that keep to these rules, and one draw needn't show every extreme that they name: `position_domain_label`: on each device the used slots come first; a device may use none. Reading the devices in order and their used slots in order lists every mesh's blocks as one run, meshes in increasing order, each mesh 2 or more blocks. Exactly 4096 slots are used in all, and some device uses all 64 of its slots. `position_vertex_tally`: 128 in every used slot except the last block of each mesh, which holds 1 to 128; 0 in unused slots.
All inputs are finite; a program needn't handle non-finite values.
Results may differ from the reference program's by a relative error of at most 0.012.
The reference program's roundings to bfloat16 on the way count: a program that leaves them out, or rounds other values in their place, can miss the bound.
Values may be sent and summed in bfloat16 or wider, within the bound.
No kernel may reach another device: no remote copies, remote signals or barrier semaphores. Data moves between devices by JAX's collectives and lax.ppermute only.
A program may use at most 128 MiB of HBM per device.

```python
import math
import jax
import jax.numpy as jnp
from jax import lax

C = 256
ATTENTION_GROUPS = 8
DH = 32
M = 64
BLOCK = 128
SLOTS = 64
OWN = 32
MESHES = 64
N_GRP = 8
N_DEV = 16
DEVICES = 128


def layout_tables(key):
    device_count = N_GRP * N_DEV
    half_count = device_count // 2
    block_total = device_count * OWN
    key_bridge, key_full, key_moves, key_heavy, key_last = jax.random.split(jax.random.fold_in(key, 7), 5)
    bridge = jax.random.randint(key_bridge, (), 0, half_count - 1).astype(jnp.int32)
    device = jnp.arange(device_count, dtype=jnp.int32)
    vacant = (device > bridge) & (device < bridge + half_count)
    active = jnp.logical_not(vacant)
    active_rank = jnp.cumsum(active.astype(jnp.int32)) - 1
    full_rank = jax.random.randint(key_full, (), 0, half_count + 1).astype(jnp.int32)
    is_full = active & (active_rank == full_rank)
    others = active & jnp.logical_not(is_full)
    other_rank = (jnp.cumsum(others.astype(jnp.int32)) - 1).astype(jnp.int32)
    share = (block_total - SLOTS) // half_count
    leftover = block_total - SLOTS - share * half_count
    base = share + (other_rank < leftover).astype(jnp.int32)
    limit = max(0, min(share // 2, SLOTS - share - 1))
    pair_moves = jax.random.randint(key_moves, (device_count,), 0, limit + 1).astype(jnp.int32)
    pair_id = jnp.clip(other_rank // 2, 0, device_count - 1)
    delta = pair_moves[pair_id]
    even = other_rank % 2 == 0
    partnered = jnp.logical_or(jnp.logical_not(even), other_rank + 1 < half_count)
    signed = jnp.where(even, delta, -delta) * partnered.astype(jnp.int32)
    used_slots = jnp.where(is_full, SLOTS, jnp.where(others, base + signed, 0)).astype(jnp.int32)
    run_ends = jnp.cumsum(used_slots).astype(jnp.int32)
    starts = run_ends - used_slots
    bridge_start = run_ends[bridge] - 1
    heavy = jax.random.randint(key_heavy, (MESHES,), 1, 9).astype(jnp.int32)
    heavy = heavy * heavy * heavy
    middle = jnp.clip(bridge_start * (MESHES - 1) // block_total, 1, MESHES - 2).astype(jnp.int32)
    index = jnp.arange(MESHES, dtype=jnp.int32)
    before = index < middle
    after = index > middle
    rest_after = block_total - bridge_start - 2
    heavy_before = jnp.sum(jnp.where(before, heavy, 0))
    heavy_after = jnp.sum(jnp.where(after, heavy, 0))
    size_before = 2 + (bridge_start - 2 * middle) * heavy // heavy_before
    size_after = 2 + (rest_after - 2 * (MESHES - 1 - middle)) * heavy // heavy_after
    mesh_blocks = jnp.where(before, size_before, jnp.where(after, size_after, 2)).astype(jnp.int32)
    short_before = bridge_start - jnp.sum(jnp.where(before, mesh_blocks, 0))
    short_after = rest_after - jnp.sum(jnp.where(after, mesh_blocks, 0))
    mesh_blocks = mesh_blocks + jnp.where(index == middle - 1, short_before, 0) + jnp.where(index == MESHES - 1, short_after, 0)
    mesh_ends = jnp.cumsum(mesh_blocks).astype(jnp.int32)
    column = jnp.arange(SLOTS, dtype=jnp.int32)[None, :]
    global_block = starts[:, None] + column
    in_use = column < used_slots[:, None]
    mesh_of = jnp.sum((mesh_ends[None, None, :] <= global_block[:, :, None]).astype(jnp.int32), axis=2)
    clipped = jnp.minimum(mesh_of, MESHES - 1)
    last_size = jax.random.randint(key_last, (MESHES,), 1, BLOCK + 1).astype(jnp.int32)
    is_last = global_block == mesh_ends[clipped] - 1
    filled = jnp.where(is_last, last_size[clipped], BLOCK)
    position_domain_label = jnp.where(in_use, mesh_of, MESHES).reshape(-1).astype(jnp.int32)
    position_vertex_tally = jnp.where(in_use, filled, 0).reshape(-1).astype(jnp.int32)
    return (position_domain_label, position_vertex_tally)


def draw_position_domain_label(key, part):
    return layout_tables(key)[0]


def draw_position_vertex_tally(key, part):
    return layout_tables(key)[1]


def draw_partition_score_matrix(key, part):
    base = jnp.clip(jax.random.normal(jax.random.fold_in(key, 11), (DH, M), jnp.float32), -3.0, 3.0) / math.sqrt(DH)
    return base.astype(jnp.bfloat16)


def draw_partition_attention_maps(key, part):
    base = jnp.clip(jax.random.normal(jax.random.fold_in(key, 17), (3, DH, DH), jnp.float32), -3.0, 3.0) / math.sqrt(DH)
    return base


def block_levels(own_key, extent, pieces, smallest, top_value):
    def one(axis_at, blocks):
        heights = jax.random.uniform(jax.random.fold_in(jax.random.fold_in(own_key, 6), axis_at), (blocks,), jnp.float32, smallest / len(pieces), top_value / len(pieces))
        return jnp.repeat(jnp.exp(heights), extent[axis_at] // blocks).reshape((-1,) + (1,) * (len(extent) - axis_at - 1))

    gain = one(*pieces[0])
    for cut in pieces[1:]:
        gain = gain * one(*cut)
    return gain


def scatter_about(stream_key, shape, scale, bound, cuts=(), held_as=jnp.bfloat16):
    gain = block_levels(stream_key, shape, cuts, -0.22, 0.18) if cuts else 1.0
    values = jax.random.normal(stream_key, shape, jnp.float32) * scale * gain
    return jnp.minimum(jnp.maximum(values, -bound), bound).astype(held_as)


def setup_inputs(seed: int = 0) -> dict:
    key_list = jax.random.split(jax.random.key(seed), 11)
    return {
        "vertex_values": scatter_about(key_list[0], (DEVICES * SLOTS, BLOCK, C), 1.0, 6.0, ((0, 128),)),
        "position_domain_label": draw_position_domain_label(jax.random.fold_in(key_list[10], 71), 0),
        "position_vertex_tally": draw_position_vertex_tally(jax.random.fold_in(key_list[10], 71), 0),
        "normalizer_gain": jnp.clip(1.0 + 0.18 * jax.random.normal(key_list[3], (C,), jnp.float32), 0.1, 1.9),
        "embedding_matrix": scatter_about(key_list[4], (C, C), C ** -0.5, 0.375),
        "partition_input_matrix": scatter_about(key_list[5], (C, C), C ** -0.5, 0.375),
        "partition_score_matrix": draw_partition_score_matrix(jax.random.fold_in(key_list[10], 71), 0),
        "softmax_sharpness": jnp.clip(jnp.exp(jax.random.uniform(key_list[7], (ATTENTION_GROUPS,), jnp.float32, math.log(0.3), math.log(1.0))), 0.3, 1.0),
        "partition_attention_maps": draw_partition_attention_maps(jax.random.fold_in(key_list[10], 71), 0),
        "readout_matrix": scatter_about(key_list[9], (C, C), (C // 16) ** -0.5, 1.5),
    }


HIGHEST_PRECISION = lax.Precision.HIGHEST

def partition_routine(tile_sequence, vertex_tallies, domain_sequence, normalizer_gain, embedding_matrix, partition_input_matrix, partition_score_matrix, softmax_sharpness):
    tile_amount, tile_height, model_width = tile_sequence.shape
    attention_group_amount = softmax_sharpness.shape[0]
    head_width = model_width // attention_group_amount
    partition_amount = partition_score_matrix.shape[1]
    flattened = tile_sequence.reshape(tile_amount * tile_height, model_width).astype(jnp.float32)
    centre = flattened - lax.optimization_barrier(jnp.mean(flattened, axis=1, keepdims=True))
    spread = lax.optimization_barrier(jnp.mean(centre * centre, axis=1, keepdims=True))
    normed = (centre * lax.rsqrt(spread + 1e-05) * normalizer_gain).astype(jnp.bfloat16)
    features = jnp.dot(normed, embedding_matrix, preferred_element_type=jnp.float32).astype(jnp.bfloat16)
    middles = jnp.dot(normed, partition_input_matrix, preferred_element_type=jnp.float32).astype(jnp.bfloat16)
    partition_scores = jnp.dot(middles.reshape(-1, head_width), partition_score_matrix, preferred_element_type=jnp.float32)
    partition_scores = partition_scores.reshape(tile_amount, tile_height, attention_group_amount, partition_amount) / softmax_sharpness[:, None]
    living = (lax.broadcasted_iota(jnp.int32, (tile_amount, tile_height), 1) < vertex_tallies[:, None]).astype(jnp.float32)
    partition_shares = (jax.nn.softmax(partition_scores, axis=-1) * living[:, :, None, None]).astype(jnp.bfloat16)
    partial_sums = jnp.einsum('bphm,bphd->bhmd', partition_shares.astype(jnp.float32), features.reshape(tile_amount, tile_height, attention_group_amount, head_width).astype(jnp.float32), precision=HIGHEST_PRECISION)
    partial_totals = lax.optimization_barrier(jnp.sum(partition_shares.astype(jnp.float32), axis=1))
    one_hot = (domain_sequence[:, None] == lax.broadcasted_iota(jnp.int32, (tile_amount, MESHES), 1)).astype(jnp.float32)
    domain_accumulated = jnp.dot(one_hot.T, partial_sums.reshape(tile_amount, -1), precision=HIGHEST_PRECISION)
    domain_share_accumulated = jnp.dot(one_hot.T, partial_totals.reshape(tile_amount, -1), precision=HIGHEST_PRECISION)
    return (partition_shares.reshape(tile_amount, tile_height, attention_group_amount * partition_amount), domain_accumulated, domain_share_accumulated)

def attend_tokens(domain_accumulated, domain_share_accumulated, partition_attention_maps):
    row_count, partition_amount = domain_share_accumulated.shape
    head_width = partition_attention_maps.shape[1]
    tokens = domain_accumulated.reshape(row_count, partition_amount, head_width) / (domain_share_accumulated[:, :, None] + 1.0)
    queries = jnp.einsum('rmd,de->rme', tokens, partition_attention_maps[0], precision=HIGHEST_PRECISION)
    key_rows = jnp.einsum('rmd,de->rme', tokens, partition_attention_maps[1], precision=HIGHEST_PRECISION)
    values = jnp.einsum('rmd,de->rme', tokens, partition_attention_maps[2], precision=HIGHEST_PRECISION)
    scores = jnp.einsum('rme,rne->rmn', queries, key_rows, precision=HIGHEST_PRECISION) * head_width ** (-0.5)
    token_probs = jax.nn.softmax(scores, axis=-1)
    blended = jnp.einsum('rmn,rne->rme', token_probs, values, precision=HIGHEST_PRECISION)
    return blended.reshape(row_count, partition_amount * head_width).astype(jnp.bfloat16)

def spread_phase(tile_sequence, vertex_tallies, domain_sequence, partition_shares, tokens, readout_matrix):
    tile_amount, tile_height, model_width = tile_sequence.shape
    attention_group_amount = tokens.shape[0] // MESHES
    partition_amount = partition_shares.shape[2] // attention_group_amount
    head_width = model_width // attention_group_amount
    tables = tokens.reshape(MESHES, attention_group_amount, partition_amount, head_width)
    chosen = jnp.take(tables, jnp.minimum(domain_sequence, MESHES - 1), axis=0)
    blended = jnp.einsum('bphm,bhmd->bphd', partition_shares.reshape(tile_amount, tile_height, attention_group_amount, partition_amount).astype(jnp.float32), chosen.astype(jnp.float32), precision=HIGHEST_PRECISION).astype(jnp.bfloat16)
    projected = jnp.dot(blended.reshape(-1, model_width), readout_matrix, preferred_element_type=jnp.float32)
    living = (lax.broadcasted_iota(jnp.int32, (tile_amount, tile_height), 1) < vertex_tallies[:, None]).astype(jnp.float32)
    result = (tile_sequence.reshape(-1, model_width).astype(jnp.float32) + projected) * living.reshape(-1, 1)
    return result.reshape(tile_amount, tile_height, model_width).astype(jnp.bfloat16)

def reference(vertex_values, position_domain_label, position_vertex_tally, normalizer_gain, embedding_matrix, partition_input_matrix, partition_score_matrix, softmax_sharpness, partition_attention_maps, readout_matrix):
    used_slots = lax.optimization_barrier(jnp.sum((position_domain_label < MESHES).astype(jnp.int32).reshape(DEVICES, SLOTS), axis=1))
    run_ends = jnp.cumsum(used_slots).astype(jnp.int32)
    starts = run_ends - used_slots
    block_total = DEVICES * OWN
    global_index = jnp.arange(block_total, dtype=jnp.int32)
    source = lax.optimization_barrier(jnp.sum((run_ends[None, :] <= global_index[:, None]).astype(jnp.int32), axis=1))
    home_rows = (source * SLOTS + global_index - starts[source]).astype(jnp.int32)
    group_count = block_total // 64
    tile_sequence = vertex_values[home_rows].reshape(group_count, 64, BLOCK, C)
    vertex_tallies = position_vertex_tally[home_rows].reshape(group_count, 64)
    domain_sequence = position_domain_label[home_rows].reshape(group_count, 64)

    def gather_step(running, lookup_element):
        vacant_position_flags, domain_accumulated, domain_share_accumulated = partition_routine(lookup_element[0], lookup_element[1], lookup_element[2], normalizer_gain, embedding_matrix, partition_input_matrix, partition_score_matrix, softmax_sharpness)
        return ((running[0] + domain_accumulated, running[1] + domain_share_accumulated), None)
    initial = (jnp.zeros((MESHES, C * M), jnp.float32), jnp.zeros((MESHES, ATTENTION_GROUPS * M), jnp.float32))
    (domain_accumulated, domain_share_accumulated), vacant_position_flags = lax.scan(gather_step, initial, (tile_sequence, vertex_tallies, domain_sequence))
    tokens = attend_tokens(domain_accumulated.reshape(MESHES * ATTENTION_GROUPS, -1), domain_share_accumulated.reshape(MESHES * ATTENTION_GROUPS, -1), partition_attention_maps)

    def spread_step(lookup_element):
        partition_shares = partition_routine(lookup_element[0], lookup_element[1], lookup_element[2], normalizer_gain, embedding_matrix, partition_input_matrix, partition_score_matrix, softmax_sharpness)[0]
        return spread_phase(lookup_element[0], lookup_element[1], lookup_element[2], partition_shares, tokens, readout_matrix)
    results = lax.map(spread_step, (tile_sequence, vertex_tallies, domain_sequence))
    return jnp.zeros_like(vertex_values).at[home_rows].set(results.reshape(block_total, BLOCK, C))
```

```python
import jax
import jax.numpy as jnp
from jax import lax
from jax.experimental import pallas as pl
from jax.experimental.pallas import tpu as pltpu
from jax.sharding import PartitionSpec as P

MESHES = 64
CHUNK = 4
LOG2E = 1.4426950408889634
AXES = ("grp", "dev")
HIGHEST = lax.Precision.HIGHEST
F32 = jnp.float32
BF16 = jnp.bfloat16


def _dot(a, b, dims, precision=None):
    return lax.dot_general(a, b, (dims, ((), ())), precision=precision, preferred_element_type=F32)


def _living(tal, base, points, block):
    lane = lax.broadcasted_iota(jnp.int32, (1, points), 1)
    limit = jnp.zeros((1, points), jnp.int32)
    for b in range(points // block):
        limit = jnp.where(lane // block == b, b * block + tal[base + b], limit)
    return (lane < limit).astype(F32)


def _last_label(lab, base):
    last = lab[base]
    for b in range(1, CHUNK):
        last = jnp.where(lab[base + b] < MESHES, lab[base + b], last)
    return last


def gather_kernel(
    lab, tal, sharp, x_ref, gain_ref, emb_ref, pin_ref, score_ref,
    w_ref, acc_ref, send_ref, meta_ref,
    wt_ref, st_ref, cs_ref,
):
    step = pl.program_id(0)
    base = step * CHUNK
    _, block, width = x_ref.shape
    points = CHUNK * block
    heads = sharp.shape[0]
    dh = width // heads
    parts = score_ref.shape[1]
    group = heads // 2

    @pl.when(step == 0)
    def _():
        wt_ref[:width, :] = emb_ref[...].astype(F32).T.astype(BF16)
        wt_ref[width:, :] = pin_ref[...].astype(F32).T.astype(BF16)
        st_ref[...] = score_ref[...].astype(F32).T.astype(BF16)
        for h in range(heads):
            cs_ref[h : h + 1, :] = jnp.full((1, points), LOG2E, F32) / jnp.full(
                (1, points), sharp[h], F32
            )
        meta_ref[0] = lab[0]
        meta_ref[1] = lab[0]

        @pl.when(lab[0] >= MESHES)
        def _():
            acc_ref[0] = jnp.zeros(acc_ref.shape[1:], F32)

    @pl.when(lab[base] < MESHES)
    def _():
        x = x_ref[...].reshape(points, width).astype(F32)
        centre = x - jnp.sum(x, axis=1, keepdims=True) * (1.0 / width)
        var = jnp.sum(centre * centre, axis=1, keepdims=True) * (1.0 / width)
        normed = (centre * lax.rsqrt(var + 1e-05) * gain_ref[...]).astype(BF16)
        both = _dot(wt_ref[...], normed, ((1,), (1,))).astype(BF16)
        live = _living(tal, base, points, block)
        for h in range(heads):
            mid = both[width + h * dh : width + (h + 1) * dh, :]
            logit = _dot(st_ref[...], mid, ((1,), (0,)))
            top = jnp.max(logit, axis=0, keepdims=True)
            e = jnp.exp2((logit - top) * cs_ref[h : h + 1, :])
            scale = live / jnp.sum(e, axis=0, keepdims=True)
            w_ref[0, h * parts : (h + 1) * parts, :] = (e * scale).astype(BF16)

        ones = jnp.ones((16, points), BF16)
        low = lab[base]
        high = _last_label(lab, base)
        meta_ref[1] = high
        lane = lax.broadcasted_iota(jnp.int32, (dh, 128), 1)

        def add(mesh, mask):
            slot = mesh - lab[0]
            fresh = jnp.logical_or(step == 0, lab[jnp.maximum(base - 1, 0)] != mesh)
            for g in range(2):
                f = jnp.concatenate([both[g * group * dh : (g + 1) * group * dh, :], ones], axis=0)
                w = w_ref[0, g * group * parts : (g + 1) * group * parts, :]
                if mask is not None:
                    f = jnp.where(mask, f, jnp.zeros_like(f))
                s = _dot(f, w, ((1,), (1,)))
                for t in range(2):
                    tile = s[:, t * 128 : (t + 1) * 128]
                    r = 2 * t * dh
                    own = jnp.where(lane < parts, tile[r : r + dh], tile[r + dh : r + 2 * dh])
                    own = jnp.concatenate([own, tile[group * dh : group * dh + 8]], axis=0)
                    at = (slot, slice(None), slice((2 * g + t) * 128, (2 * g + t + 1) * 128))
                    acc_ref[at] = jnp.where(fresh, own, acc_ref[at] + own)

        @pl.when(low == high)
        def _():
            add(low, None)

        @pl.when(low != high)
        def _():
            where = lax.broadcasted_iota(jnp.int32, (group * dh + 16, points), 1) // block
            which = jnp.full(where.shape, MESHES, jnp.int32)
            for b in range(CHUNK):
                which = jnp.where(where == b, lab[base + b], which)

            @pl.loop(low, high + 1)
            def _(mesh):
                add(mesh, which == mesh)

    @pl.when(step == pl.num_programs(0) - 1)
    def _():
        last = meta_ref[1] - lab[0]
        alone = last == 0
        column = lax.broadcasted_iota(jnp.int32, (128, 128), 1)
        tail = jnp.where(alone, -1, meta_ref[1]).astype(F32)
        send_ref[:, 512:640] = jnp.where(column == 0, lab[0].astype(F32), tail)
        for t in range(4):
            cut = slice(t * 128, (t + 1) * 128)
            row = slice(t * dh, (t + 1) * dh)
            head = acc_ref[0, :, cut]
            foot = acc_ref[last, :, cut]
            foot = jnp.where(alone, jnp.zeros_like(foot), foot)
            send_ref[row, 0:128] = head[:dh]
            send_ref[row, 128:256] = foot[:dh]
            send_ref[row, 256:384] = jnp.broadcast_to(head[dh : dh + 1], (dh, 128))
            send_ref[row, 384:512] = jnp.broadcast_to(foot[dh : dh + 1], (dh, 128))


def owner_kernel(r_ref, o_ref):
    labels = r_ref[:, 512:640]
    first = labels[:, 0:1]
    final = labels[:, 1:2]
    rows = jnp.concatenate([first, final], axis=0)
    rows = jnp.broadcast_to(rows, (256, 256))
    same = (rows == rows.T).astype(F32)
    data = jnp.concatenate(
        [
            jnp.concatenate([r_ref[:, 0:128], r_ref[:, 256:384]], axis=1),
            jnp.concatenate([r_ref[:, 128:256], r_ref[:, 384:512]], axis=1),
        ],
        axis=0,
    )
    whole = _dot(same, data, ((1,), (0,)), HIGHEST)
    tokens = whole[:, :128] / (whole[:, 128:] + 1.0)
    o_ref[:, 0:128] = tokens[:128]
    o_ref[:, 128:256] = tokens[128:]


def spread_kernel(
    lab, tal, meta, x_ref, w_ref, acc_ref, tok_ref, maps_ref, out_proj_ref,
    o_ref,
    mix_ref,
):
    step = pl.program_id(0)
    base = step * CHUNK
    _, block, width = x_ref.shape
    points = CHUNK * block
    dh = maps_ref.shape[1]
    heads = width // dh
    group = heads // 2
    parts = w_ref.shape[1] // heads
    first = meta[0]
    last = meta[1]

    @pl.when(jnp.logical_and(step == 0, first < MESHES))
    def _():
        row = lax.broadcasted_iota(jnp.int32, (128, 128), 0) // parts
        col = lax.broadcasted_iota(jnp.int32, (128, 128), 1) // parts
        paired = row == col
        lane = lax.broadcasted_iota(jnp.int32, (dh, 128), 1)
        mapt = [maps_ref[i].T for i in range(3)]

        @pl.loop(0, last - first + 1)
        def _(slot):
            for t in range(4):
                cut = slice(t * 128, (t + 1) * 128)
                kept = acc_ref[slot, :, cut]
                token = kept[:dh] / (kept[dh : dh + 1] + 1.0)
                token = jnp.where(slot == last - first, tok_ref[t * dh : (t + 1) * dh, 128:256], token)
                token = jnp.where(slot == 0, tok_ref[t * dh : (t + 1) * dh, 0:128], token)
                q, k, v = (_dot(m, token, ((1,), (0,)), HIGHEST) for m in mapt)
                score = _dot(k.T, q, ((1,), (0,)), HIGHEST) * (dh**-0.5 * LOG2E)
                score = jnp.where(paired, score, -1e38)
                e = jnp.exp2(score - jnp.max(score, axis=0, keepdims=True))
                prob = e / jnp.sum(e, axis=0, keepdims=True)
                mixed = _dot(v, prob, ((1,), (0,)), HIGHEST)
                for s in range(2):
                    own = jnp.where(lane // parts == s, mixed, 0.0).astype(BF16)
                    r = ((2 * t + s) % group) * dh
                    c = (t % 2) * 128
                    mix_ref[slot, t // 2, r : r + dh, c : c + 128] = own
                    mix_ref[slot, t // 2, r : r + dh, 128 - c : 256 - c] = jnp.zeros_like(own)

    @pl.when(lab[base] >= MESHES)
    def _():
        o_ref[...] = jnp.zeros(o_ref.shape, BF16)

    @pl.when(lab[base] < MESHES)
    def _():
        low = lab[base]
        high = _last_label(lab, base)
        rows = group * parts

        def finish(spread, x, live):
            projected = _dot(spread, out_proj_ref[...], ((0,), (0,)))
            return ((x.astype(F32) + projected) * live).astype(BF16)

        def alive(limit, count):
            point = lax.broadcasted_iota(jnp.int32, (count, width), 0)
            return point < limit

        @pl.when(low == high)
        def _():
            slot = low - first
            spread = jnp.concatenate(
                [
                    _dot(mix_ref[slot, g], w_ref[0, g * rows : (g + 1) * rows, :], ((1,), (0,)))
                    for g in range(2)
                ],
                axis=0,
            ).astype(BF16)
            projected = _dot(spread, out_proj_ref[...], ((0,), (0,)))
            for b in range(CHUNK):
                whole = x_ref[b].astype(F32) + projected[b * block : (b + 1) * block]
                o_ref[b] = jnp.where(alive(tal[base + b], block), whole, 0.0).astype(BF16)

        @pl.when(low != high)
        def _():
            for b in range(CHUNK):
                slot = jnp.minimum(lab[base + b], high) - first
                cut = slice(b * block, (b + 1) * block)
                spread = jnp.concatenate(
                    [
                        _dot(mix_ref[slot, g], w_ref[0, g * rows : (g + 1) * rows, cut], ((1,), (0,)))
                        for g in range(2)
                    ],
                    axis=0,
                ).astype(BF16)
                projected = _dot(spread, out_proj_ref[...], ((0,), (0,)))
                whole = x_ref[b].astype(F32) + projected
                o_ref[b] = jnp.where(alive(tal[base + b], block), whole, 0.0).astype(BF16)


def on_device(
    vertex_values,
    position_domain_label,
    position_vertex_tally,
    normalizer_gain,
    embedding_matrix,
    partition_input_matrix,
    partition_score_matrix,
    softmax_sharpness,
    partition_attention_maps,
    readout_matrix,
):
    slots, block, width = vertex_values.shape
    heads = softmax_sharpness.shape[0]
    dh, parts = partition_score_matrix.shape
    steps = slots // CHUNK
    points = CHUNK * block
    local = slots // 2 + 1
    local = local + 1
    whole = lambda *shape: pl.BlockSpec(shape, lambda i, *_: (0,) * len(shape))
    chunk = pl.BlockSpec((CHUNK, block, width), lambda i, *_: (i, 0, 0))
    weight = pl.BlockSpec((1, heads * parts, points), lambda i, *_: (i, 0, 0))
    shares, sums, send, meta = pl.pallas_call(
        gather_kernel,
        name="gather",
        grid_spec=pltpu.PrefetchScalarGridSpec(
            num_scalar_prefetch=3,
            grid=(steps,),
            in_specs=[
                chunk,
                whole(1, width),
                whole(width, width),
                whole(width, width),
                whole(dh, parts),
            ],
            out_specs=[
                weight,
                whole(local, dh + 8, heads * parts),
                whole(128, 640),
                pl.BlockSpec(memory_space=pltpu.SMEM),
            ],
            scratch_shapes=[
                pltpu.VMEM((2 * width, width), BF16),
                pltpu.VMEM((parts, dh), BF16),
                pltpu.VMEM((heads, points), F32),
            ],
        ),
        out_shape=[
            jax.ShapeDtypeStruct((steps, heads * parts, points), BF16),
            jax.ShapeDtypeStruct((local, dh + 8, heads * parts), F32),
            jax.ShapeDtypeStruct((128, 640), F32),
            jax.ShapeDtypeStruct((8,), jnp.int32),
        ],
        compiler_params=pltpu.CompilerParams(dimension_semantics=("arbitrary",)),
    )(
        position_domain_label,
        position_vertex_tally,
        softmax_sharpness,
        vertex_values,
        normalizer_gain.reshape(1, width),
        embedding_matrix,
        partition_input_matrix,
        partition_score_matrix,
    )
    got = lax.all_to_all(send, AXES, 0, 0, tiled=True)
    back = pl.pallas_call(
        owner_kernel, name="owner", out_shape=jax.ShapeDtypeStruct((128, 256), F32)
    )(got)
    tokens = lax.all_to_all(back, AXES, 0, 0, tiled=True)
    return pl.pallas_call(
        spread_kernel,
        name="spread",
        grid_spec=pltpu.PrefetchScalarGridSpec(
            num_scalar_prefetch=3,
            grid=(steps,),
            in_specs=[
                chunk,
                weight,
                whole(local, dh + 8, heads * parts),
                whole(128, 256),
                whole(3, dh, dh),
                whole(width, width),
            ],
            out_specs=chunk,
            scratch_shapes=[pltpu.VMEM((local, 2, width // 2, heads * parts // 2), BF16)],
        ),
        out_shape=jax.ShapeDtypeStruct(vertex_values.shape, BF16),
        compiler_params=pltpu.CompilerParams(dimension_semantics=("arbitrary",)),
    )(
        position_domain_label,
        position_vertex_tally,
        meta,
        vertex_values,
        shares,
        sums,
        tokens,
        partition_attention_maps,
        readout_matrix,
    )


def solution(mesh):
    rows = P(AXES)
    return jax.shard_map(
        on_device,
        mesh=mesh,
        in_specs=(P(AXES, None, None), rows, rows, P(), P(), P(), P(), P(), P(), P()),
        out_specs=P(AXES, None, None),
        check_vma=False,
    )
```

```python
import jax
import jax.numpy as jnp
from jax import lax
from jax.experimental import pallas as pl
from jax.experimental.pallas import tpu as pltpu
from jax.sharding import PartitionSpec as P

MESHES = 64
UNIT = 4
PIECE = 4
BATCH = 4
LOG2E = 1.4426950408889634
AXES = ("grp", "dev")
F32 = jnp.float32
BF16 = jnp.bfloat16
HIGHEST = lax.Precision.HIGHEST


def _dot(a, b, dims, precision=None):
    return lax.dot_general(a, b, (dims, ((), ())), precision=precision, preferred_element_type=F32)


def _split(a, terms):
    out = []
    for _ in range(terms):
        out.append(a.astype(BF16))
        a = a - out[-1].astype(F32)
    return out


def _dot3(a, b):
    ah, al = _split(a, 2)
    bh, bl = _split(b, 2)
    return _dot(
        jnp.concatenate([ah, al, ah], axis=1), jnp.concatenate([bh, bh, bl], axis=0), ((1,), (0,))
    )


def _units(lab, start, slot, blocks):
    def visit(b, carry):
        count, begin = carry
        mesh = lab[b]
        before = lab[jnp.maximum(b - 1, 0)]
        opens = jnp.logical_or(jnp.logical_or(b == 0, mesh != before), b - begin == UNIT)
        opens = jnp.logical_and(opens, mesh < MESHES)

        @pl.when(opens)
        def _():
            start[count] = b
            slot[count] = mesh - lab[0]

        return count + opens.astype(jnp.int32), jnp.where(opens, b, begin)

    used = jnp.int32(0)
    for b in range(blocks):
        used = used + (lab[b] < MESHES).astype(jnp.int32)
    count, _ = lax.fori_loop(0, blocks, visit, (jnp.int32(0), jnp.int32(0)))
    return count, used


def gather_kernel(
    lab, tal, sharp, x_hbm, gain_hbm, emb_hbm, pin_hbm, score_hbm,
    x_ref, w_ref, acc_ref, send_ref, start, slot, meta,
    gain_ref, emb_ref, pin_ref, score_ref, wt_ref, st_ref, mean_ref, f_ref, sems, param_sems,
):
    blocks, block, width = x_hbm.shape
    points = UNIT * block
    heads = sharp.shape[0]
    dh = width // heads
    parts = score_ref.shape[1]
    group = heads // 2
    spare = acc_ref.shape[0] - 1
    pieces = blocks // PIECE

    def copy(i):
        part = pl.ds(i * PIECE, PIECE)
        return pltpu.make_async_copy(x_hbm.at[part], x_ref.at[part], sems.at[i])

    given = ((gain_hbm, gain_ref), (emb_hbm, emb_ref), (pin_hbm, pin_ref), (score_hbm, score_ref))
    params = [pltpu.make_async_copy(a, b, param_sems.at[n]) for n, (a, b) in enumerate(given)]
    for p in params:
        p.start()
    for i in range(pieces):
        copy(i).start()
    row = lax.broadcasted_iota(jnp.int32, (width, width), 0)
    col = lax.broadcasted_iota(jnp.int32, (width, width), 1)
    mean_ref[...] = ((row == col).astype(F32) - 1.0 / width).astype(BF16)
    count, used = _units(lab, start, slot, blocks)
    start[count] = used
    for n in range(BATCH):
        start[count + 1 + n] = blocks
        slot[count + n] = spare
    meta[0] = lab[0]
    meta[1] = count
    meta[2] = used
    last = jnp.where(used > 0, slot[jnp.maximum(count - 1, 0)], 0)
    meta[3] = last
    for p in params:
        p.wait()
    gain_ref[...] = gain_ref[...] * width**0.5
    wt_ref[:width, :] = emb_ref[...].astype(F32).T.astype(BF16)
    wt_ref[width:, :] = pin_ref[...].astype(F32).T.astype(BF16)
    score = score_ref[...].astype(F32).T
    for h in range(heads):
        factor = jnp.full(score.shape, LOG2E, F32) / jnp.full(score.shape, sharp[h], F32)
        st_ref[h] = jnp.concatenate(_split(score * factor, 3), axis=1)

    group_points = group * dh
    ones = jnp.ones((16, block), BF16)
    lane = lax.broadcasted_iota(jnp.int32, (dh, 128), 1)

    def normalize(s):
        x = x_ref[pl.ds(s, UNIT)].reshape(points, width)
        centre = _dot(x, mean_ref[...], ((1,), (0,)))
        return centre

    def scale(centre):
        square = jnp.sum(centre * centre, axis=1, keepdims=True)
        return (centre * lax.rsqrt(square + 1e-05 * width) * gain_ref[...]).astype(BF16)

    def weigh(logit, live):
        e = jnp.exp2(logit - jnp.max(logit, axis=0, keepdims=True))
        return (e * (live / jnp.sum(e, axis=0, keepdims=True))).astype(BF16)

    def living(s):
        spot = lax.broadcasted_iota(jnp.int32, (1, points), 1)
        limit = jnp.zeros((1, points), jnp.int32)
        for b in range(UNIT):
            limit = jnp.where(spot // block == b, b * block + tal[s + b], limit)
        return (spot < limit).astype(F32)

    def put(ref, s, row, value):
        for b in range(UNIT):
            ref[s + b, row : row + value.shape[0], :] = value[:, b * block : (b + 1) * block]

    for i in range(pieces):
        copy(i).wait()

    trips = (used + BATCH * UNIT - 1) // (BATCH * UNIT)

    @pl.loop(0, trips)
    def _(j):
        first = [(j * BATCH + n) * UNIT for n in range(BATCH)]
        centres = [normalize(s) for s in first]
        normed = [scale(c) for c in centres]
        both = [_dot(wt_ref[...], n, ((1,), (1,))).astype(BF16) for n in normed]
        for s, a in zip(first, both):
            put(f_ref, s, 0, a[:width])
        lives = [living(s) for s in first]
        items = [(h, n) for h in range(heads) for n in range(BATCH)]
        ahead = {}
        for at in range(len(items) + BATCH):
            if at < len(items):
                h, n = items[at]
                mid = both[n][width + h * dh : width + (h + 1) * dh, :]
                ahead[h, n] = _dot(st_ref[h], jnp.concatenate([mid, mid, mid], axis=0), ((1,), (0,)))
            if at >= BATCH:
                h, n = items[at - BATCH]
                put(w_ref, first[n], h * parts, weigh(ahead.pop((h, n)), lives[n]))

    for b in range(UNIT):
        w_ref[trips * BATCH * UNIT + b] = jnp.zeros(w_ref.shape[1:], BF16)

    def product(n, g):
        s = start[n]
        f = []
        for b in range(UNIT):
            part = jnp.concatenate([f_ref[s + b, g * group_points : (g + 1) * group_points], ones], axis=0)
            f.append(jnp.where(s + b < start[n + 1], part, jnp.zeros_like(part)))
        rows = slice(g * group * parts, (g + 1) * group * parts)
        w = jnp.concatenate([w_ref[s + b, rows] for b in range(UNIT)], axis=1)
        return _dot(jnp.concatenate(f, axis=1), w, ((1,), (1,)))

    @pl.loop(0, (count + BATCH - 1) // BATCH)
    def _(j):
        units = [j * BATCH + n for n in range(BATCH)]
        totals = [(n, g, product(n, g)) for n in units for g in range(2)]
        for n, g, total in totals:
            here = slot[n]
            fresh = jnp.logical_or(n == 0, slot[jnp.maximum(n - 1, 0)] != here)
            for t in range(2):
                tile = total[:, t * 128 : (t + 1) * 128]
                r = 2 * t * dh
                own = jnp.where(lane < parts, tile[r : r + dh], tile[r + dh : r + 2 * dh])
                own = jnp.concatenate([own, tile[group_points : group_points + 8]], axis=0)
                at = (here, slice(None), slice((2 * g + t) * 128, (2 * g + t + 1) * 128))
                acc_ref[at] = jnp.where(fresh, own, acc_ref[at] + own)

    @pl.when(used == 0)
    def _():
        acc_ref[0] = jnp.zeros(acc_ref.shape[1:], F32)

    alone = last == 0
    column = lax.broadcasted_iota(jnp.int32, (128, 128), 1)
    tail = jnp.where(alone, -1, lab[0] + last).astype(F32)
    send_ref[:, 512:640] = jnp.where(column == 0, lab[0].astype(F32), tail)
    for t in range(4):
        cut = slice(t * 128, (t + 1) * 128)
        at = slice(t * dh, (t + 1) * dh)
        head = acc_ref[0, :, cut]
        foot = acc_ref[last, :, cut]
        foot = jnp.where(alone, jnp.zeros_like(foot), foot)
        send_ref[at, 0:128] = head[:dh]
        send_ref[at, 128:256] = foot[:dh]
        send_ref[at, 256:384] = jnp.broadcast_to(head[dh : dh + 1], (dh, 128))
        send_ref[at, 384:512] = jnp.broadcast_to(foot[dh : dh + 1], (dh, 128))


def owner_kernel(r_ref, o_ref):
    labels = r_ref[:, 512:640]
    rows = jnp.concatenate([labels[:, 0:1], labels[:, 1:2]], axis=0)
    rows = jnp.broadcast_to(rows, (256, 256))
    same = (rows == rows.T).astype(F32)
    data = jnp.concatenate(
        [
            jnp.concatenate([r_ref[:, 0:128], r_ref[:, 256:384]], axis=1),
            jnp.concatenate([r_ref[:, 128:256], r_ref[:, 384:512]], axis=1),
        ],
        axis=0,
    )
    whole = _dot(same, data, ((1,), (0,)), HIGHEST)
    tokens = whole[:, :128] / (whole[:, 128:] + 1.0)
    o_ref[:, 0:128] = tokens[:128]
    o_ref[:, 128:256] = tokens[128:]


def spread_kernel(
    tal, start, slot, meta, x_ref, w_ref, acc_ref, tok_ref, maps_ref, out_proj_ref,
    o_hbm,
    o_ref, mix_ref, sems,
):
    blocks, block, width = o_hbm.shape
    dh = maps_ref.shape[1]
    heads = width // dh
    group = heads // 2
    parts = w_ref.shape[1] // heads
    rows = group * parts
    count = meta[1]
    used = meta[2]
    last = meta[3]
    pieces = blocks // PIECE
    spare = mix_ref.shape[0] - 1

    def copy(i):
        part = pl.ds(i * PIECE, PIECE)
        return pltpu.make_async_copy(o_ref.at[part], o_hbm.at[part], sems.at[i])

    def attend(ats):
        row = lax.broadcasted_iota(jnp.int32, (128, 128), 0) // parts
        col = lax.broadcasted_iota(jnp.int32, (128, 128), 1) // parts
        lane = lax.broadcasted_iota(jnp.int32, (dh, 128), 1)
        maps = jnp.concatenate([maps_ref[i].T for i in range(3)], axis=0)
        projected = []
        for at in ats:
            tokens = []
            for t in range(4):
                kept = acc_ref[at, :, t * 128 : (t + 1) * 128]
                token = kept[:dh] / (kept[dh : dh + 1] + 1.0)
                token = jnp.where(at == last, tok_ref[t * dh : (t + 1) * dh, 128:256], token)
                tokens.append(jnp.where(at == 0, tok_ref[t * dh : (t + 1) * dh, 0:128], token))
            projected.append(_dot3(maps, jnp.concatenate(tokens, axis=1)))
        tiles = [(n, t) for n in range(len(ats)) for t in range(4)]
        scores = []
        for n, t in tiles:
            q, k = (projected[n][i * dh : (i + 1) * dh, t * 128 : (t + 1) * 128] for i in range(2))
            kh, kl = _split(k * (dh**-0.5 * LOG2E), 2)
            qh, ql = _split(q, 2)
            left = jnp.concatenate([kh, kl, kh], axis=0)
            scores.append(_dot(left, jnp.concatenate([qh, qh, ql], axis=0), ((0,), (0,))))
        probs = []
        for score in scores:
            score = jnp.where(row == col, score, -1e38)
            e = jnp.exp2(score - jnp.max(score, axis=0, keepdims=True))
            probs.append(e / jnp.sum(e, axis=0, keepdims=True))
        mixes = [
            _dot3(projected[n][2 * dh :, t * 128 : (t + 1) * 128], prob)
            for (n, t), prob in zip(tiles, probs)
        ]
        for (n, t), mixed in zip(tiles, mixes):
            for s in range(2):
                own = jnp.where(lane // parts == s, mixed, 0.0).astype(BF16)
                r = ((2 * t + s) % group) * dh
                c = (t % 2) * 128
                mix_ref[ats[n], t // 2, r : r + dh, c : c + 128] = own
                mix_ref[ats[n], t // 2, r : r + dh, 128 - c : 256 - c] = jnp.zeros_like(own)

    def blend(n):
        s = start[n]
        return jnp.concatenate(
            [
                _dot(
                    mix_ref[slot[n], g],
                    jnp.concatenate([w_ref[s + b, g * rows : (g + 1) * rows] for b in range(UNIT)], axis=1),
                    ((1,), (0,)),
                )
                for g in range(2)
            ],
            axis=0,
        ).astype(BF16)

    def finish(n, mixed):
        s = start[n]
        point = lax.broadcasted_iota(jnp.int32, (block, width), 0)
        projected = _dot(mixed, out_proj_ref[...], ((0,), (0,)))
        for b in range(UNIT):
            whole = x_ref[s + b].astype(F32) + projected[b * block : (b + 1) * block]
            live = point < tal[jnp.minimum(s + b, blocks - 1)]
            o_ref[s + b] = jnp.where(live, whole, 0.0).astype(BF16)

    @pl.loop(used // PIECE * PIECE, blocks)
    def _(b):
        o_ref[b] = jnp.zeros((block, width), BF16)

    idle = (used + PIECE - 1) // PIECE

    @pl.when(used > 0)
    def _():
        @pl.loop(0, (last + 2) // 2)
        def _(j):
            attend([2 * j, jnp.where(2 * j + 1 > last, spare, 2 * j + 1)])

    def step(j, sent):
        units = [BATCH * j + n for n in range(BATCH)]
        mixed = [blend(n) for n in units]
        for n, m in zip(units, mixed):
            finish(n, m)
        final = start[jnp.minimum(BATCH * (j + 1), count)]
        final = jnp.where(final == used, idle, final // PIECE)

        @pl.loop(sent, final)
        def _(i):
            copy(i).start()

        return final

    lax.fori_loop(0, (count + BATCH - 1) // BATCH, step, jnp.int32(0))

    @pl.loop(idle, pieces)
    def _(i):
        copy(i).start()

    for i in range(pieces):
        copy(i).wait()


def on_device(
    vertex_values,
    position_domain_label,
    position_vertex_tally,
    normalizer_gain,
    embedding_matrix,
    partition_input_matrix,
    partition_score_matrix,
    softmax_sharpness,
    partition_attention_maps,
    readout_matrix,
):
    slots, block, width = vertex_values.shape
    heads = softmax_sharpness.shape[0]
    dh, parts = partition_score_matrix.shape
    points = UNIT * block
    pieces = slots // PIECE
    room = slots + UNIT
    local = slots // 2 + 2
    smem = pl.BlockSpec(memory_space=pltpu.SMEM)
    vmem = pl.BlockSpec(memory_space=pltpu.VMEM)
    hbm = pl.BlockSpec(memory_space=pltpu.HBM)
    params = pltpu.CompilerParams(vmem_limit_bytes=24 << 20)
    far = lambda a: pltpu.with_memory_space_constraint(a, pltpu.HBM)
    x, shares, sums, send, start, slot, meta = pl.pallas_call(
        gather_kernel,
        name="gather",
        in_specs=[smem, smem, smem, hbm, hbm, hbm, hbm, hbm],
        out_specs=[vmem, vmem, vmem, vmem, smem, smem, smem],
        out_shape=[
            pltpu.VMEM((room, block, width), BF16),
            pltpu.VMEM((room, heads * parts, block), BF16),
            pltpu.VMEM((local, dh + 8, heads * parts), F32),
            jax.ShapeDtypeStruct((128, 640), F32),
            jax.ShapeDtypeStruct((2 * slots,), jnp.int32),
            jax.ShapeDtypeStruct((2 * slots,), jnp.int32),
            jax.ShapeDtypeStruct((8,), jnp.int32),
        ],
        scratch_shapes=[
            pltpu.VMEM((1, width), F32),
            pltpu.VMEM((width, width), BF16),
            pltpu.VMEM((width, width), BF16),
            pltpu.VMEM((dh, parts), BF16),
            pltpu.VMEM((2 * width, width), BF16),
            pltpu.VMEM((heads, parts, 3 * dh), BF16),
            pltpu.VMEM((width, width), BF16),
            pltpu.VMEM((room, width, block), BF16),
            pltpu.SemaphoreType.DMA((pieces,)),
            pltpu.SemaphoreType.DMA((4,)),
        ],
        compiler_params=params,
    )(
        far(position_domain_label),
        far(position_vertex_tally),
        far(softmax_sharpness),
        far(vertex_values),
        far(normalizer_gain.reshape(1, width)),
        far(embedding_matrix),
        far(partition_input_matrix),
        far(partition_score_matrix),
    )
    got = lax.all_to_all(send, AXES, 0, 0, tiled=True)
    back = pl.pallas_call(
        owner_kernel,
        name="owner",
        out_shape=jax.ShapeDtypeStruct((128, 256), F32),
        compiler_params=params,
    )(got)
    tokens = lax.all_to_all(back, AXES, 0, 0, tiled=True)
    keep = lambda a: pltpu.with_memory_space_constraint(a, pltpu.VMEM)
    return pl.pallas_call(
        spread_kernel,
        name="spread",
        in_specs=[smem, smem, smem, smem, vmem, vmem, vmem, vmem, vmem, vmem],
        out_specs=hbm,
        out_shape=jax.ShapeDtypeStruct(vertex_values.shape, BF16),
        scratch_shapes=[
            pltpu.VMEM((room, block, width), BF16),
            pltpu.VMEM((local, 2, width // 2, heads * parts // 2), BF16),
            pltpu.SemaphoreType.DMA((pieces,)),
        ],
        compiler_params=params,
    )(
        position_vertex_tally,
        start,
        slot,
        meta,
        keep(x),
        keep(shares),
        keep(sums),
        tokens,
        partition_attention_maps,
        readout_matrix,
    )


def solution(mesh):
    rows = P(AXES)
    return jax.shard_map(
        on_device,
        mesh=mesh,
        in_specs=(P(AXES, None, None), rows, rows, P(), P(), P(), P(), P(), P(), P()),
        out_specs=P(AXES, None, None),
        check_vma=False,
    )
```

```python
import jax
import jax.numpy as jnp
from jax import lax
from jax.experimental import pallas as pl
from jax.experimental.pallas import tpu as pltpu
from jax.sharding import PartitionSpec as P

MESHES = 64
UNIT = 4
PIECE = 4
BATCH = 4
WIDE = 8
LOG2E = 1.4426950408889634
AXES = ("grp", "dev")
F32 = jnp.float32
BF16 = jnp.bfloat16
HIGHEST = lax.Precision.HIGHEST


def _dot(a, b, dims, precision=None):
    return lax.dot_general(a, b, (dims, ((), ())), precision=precision, preferred_element_type=F32)


def _split(a, terms):
    out = []
    for _ in range(terms):
        out.append(a.astype(BF16))
        a = a - out[-1].astype(F32)
    return out


def _dot3(a, b):
    ah, al = _split(a, 2)
    bh, bl = _split(b, 2)
    return _dot(
        jnp.concatenate([ah, al, ah], axis=1), jnp.concatenate([bh, bh, bl], axis=0), ((1,), (0,))
    )


def _units(lab, start, slot, blocks):
    count = jnp.int32(0)
    begin = jnp.int32(0)
    used = jnp.int32(0)
    for b in range(blocks):
        mesh = lab[b]
        in_use = mesh < MESHES
        opens = b - begin == UNIT
        opens = jnp.logical_or(opens, mesh != lab[b - 1]) if b else jnp.bool_(True)
        opens = jnp.logical_and(opens, in_use)
        start[count] = b
        slot[count] = mesh - lab[0]
        begin = jnp.where(opens, b, begin)
        count = count + opens.astype(jnp.int32)
        used = used + in_use.astype(jnp.int32)
    return count, used


def gather_kernel(
    lab_hbm, tal_hbm, sharp_hbm, x_hbm, gain_hbm, emb_hbm, pin_hbm, score_hbm,
    x_ref, w_ref, acc_ref, send_ref, start, slot, meta,
    lab, tal, sharp, gain_ref, emb_ref, pin_ref, score_ref, wt_ref, st_ref, mean_ref, f_ref, sems, param_sems,
):
    blocks, block, width = x_hbm.shape
    points = UNIT * block
    heads = sharp.shape[0]
    dh = width // heads
    parts = score_ref.shape[1]
    group = heads // 2
    spare = acc_ref.shape[0] - 1
    pieces = blocks // PIECE

    def copy(i):
        part = pl.ds(i * PIECE, PIECE)
        return pltpu.make_async_copy(x_hbm.at[part], x_ref.at[part], sems.at[i])

    given = (
        (lab_hbm, lab),
        (tal_hbm, tal),
        (sharp_hbm, sharp),
        (gain_hbm, gain_ref),
        (emb_hbm, emb_ref),
        (pin_hbm, pin_ref),
        (score_hbm, score_ref),
    )
    params = [pltpu.make_async_copy(a, b, param_sems.at[n]) for n, (a, b) in enumerate(given)]
    for p in params:
        p.start()
    for i in range(pieces):
        copy(i).start()
    row = lax.broadcasted_iota(jnp.int32, (width, width), 0)
    col = lax.broadcasted_iota(jnp.int32, (width, width), 1)
    mean_ref[...] = ((row == col).astype(F32) - 1.0 / width).astype(BF16)
    for p in params[:3]:
        p.wait()
    count, used = _units(lab, start, slot, blocks)
    start[count] = used
    for n in range(BATCH):
        start[count + 1 + n] = blocks
        slot[count + n] = spare
    meta[0] = lab[0]
    meta[1] = count
    meta[2] = used
    last = jnp.where(used > 0, slot[jnp.maximum(count - 1, 0)], 0)
    meta[3] = last
    for p in params[3:]:
        p.wait()
    gain_ref[...] = gain_ref[...] * width**0.5
    wt_ref[:width, :] = emb_ref[...].astype(F32).T.astype(BF16)
    wt_ref[width:, :] = pin_ref[...].astype(F32).T.astype(BF16)
    score = score_ref[...].astype(F32).T
    for h in range(heads):
        factor = jnp.full(score.shape, LOG2E, F32) / jnp.full(score.shape, sharp[h], F32)
        st_ref[h] = jnp.concatenate(_split(score * factor, 3), axis=1)

    group_points = group * dh
    ones = jnp.ones((16, block), BF16)
    lane = lax.broadcasted_iota(jnp.int32, (dh, 128), 1)

    def normalize(s):
        x = x_ref[pl.ds(s, UNIT)].reshape(points, width)
        centre = _dot(x, mean_ref[...], ((1,), (0,)))
        return centre

    def scale(centre):
        square = jnp.sum(centre * centre, axis=1, keepdims=True)
        return (centre * lax.rsqrt(square + 1e-05 * width) * gain_ref[...]).astype(BF16)

    def weigh(logit, live):
        e = jnp.exp2(logit - jnp.max(logit, axis=0, keepdims=True))
        return (e * (live / jnp.sum(e, axis=0, keepdims=True))).astype(BF16)

    def living(s):
        spot = lax.broadcasted_iota(jnp.int32, (1, points), 1)
        limit = jnp.zeros((1, points), jnp.int32)
        for b in range(UNIT):
            limit = jnp.where(spot // block == b, b * block + tal[s + b], limit)
        return (spot < limit).astype(F32)

    def put(ref, s, row, value):
        for b in range(UNIT):
            ref[s + b, row : row + value.shape[0], :] = value[:, b * block : (b + 1) * block]

    stride = WIDE * UNIT
    trips = (used + stride - 1) // stride

    @pl.loop(0, trips)
    def _(j):
        for i in range(stride // PIECE):
            copy(j * (stride // PIECE) + i).wait()
        first = [j * stride + n * UNIT for n in range(WIDE)]
        centres, normed, both = {}, {}, {}

        def project(pair):
            def embed(n):
                both[n] = _dot(wt_ref[...], normed.pop(n), ((1,), (1,))).astype(BF16)
                put(f_ref, first[n], 0, both[n][:width])

            steps = [lambda n=n: centres.__setitem__(n, normalize(first[n])) for n in pair]
            steps += [lambda n=n: normed.__setitem__(n, scale(centres.pop(n))) for n in pair]
            return steps + [lambda n=n: embed(n) for n in pair]

        pairs = [(n, n + 1) for n in range(0, WIDE, 2)]
        for step in project(pairs[0]):
            step()
        for at, pair in enumerate(pairs):
            coming = project(pairs[at + 1]) if at + 1 < len(pairs) else []
            lives = {n: living(first[n]) for n in pair}
            items = [(h, n) for h in range(heads) for n in pair]
            due = [int(0.8 * k * (len(items) + 2) / max(1, len(coming))) for k in range(len(coming))]
            ahead = {}
            for k in range(len(items) + 2):
                if k < len(items):
                    h, n = items[k]
                    mid = both[n][width + h * dh : width + (h + 1) * dh, :]
                    ahead[h, n] = _dot(st_ref[h], jnp.concatenate([mid, mid, mid], axis=0), ((1,), (0,)))
                for step, when in zip(coming, due):
                    if when == k:
                        step()
                if k >= 2:
                    h, n = items[k - 2]
                    put(w_ref, first[n], h * parts, weigh(ahead.pop((h, n)), lives[n]))

    @pl.loop(trips * (stride // PIECE), pieces)
    def _(i):
        copy(i).wait()

    for b in range(UNIT):
        w_ref[trips * stride + b] = jnp.zeros(w_ref.shape[1:], BF16)

    def product(n, g):
        s = start[n]
        f = []
        for b in range(UNIT):
            part = jnp.concatenate([f_ref[s + b, g * group_points : (g + 1) * group_points], ones], axis=0)
            f.append(jnp.where(s + b < start[n + 1], part, jnp.zeros_like(part)))
        rows = slice(g * group * parts, (g + 1) * group * parts)
        w = jnp.concatenate([w_ref[s + b, rows] for b in range(UNIT)], axis=1)
        return _dot(jnp.concatenate(f, axis=1), w, ((1,), (1,)))

    @pl.loop(0, (count + BATCH - 1) // BATCH)
    def _(j):
        units = [j * BATCH + n for n in range(BATCH)]
        totals = [(n, g, product(n, g)) for n in units for g in range(2)]
        for n, g, total in totals:
            here = slot[n]
            fresh = jnp.logical_or(n == 0, slot[jnp.maximum(n - 1, 0)] != here)
            for t in range(2):
                tile = total[:, t * 128 : (t + 1) * 128]
                r = 2 * t * dh
                own = jnp.where(lane < parts, tile[r : r + dh], tile[r + dh : r + 2 * dh])
                own = jnp.concatenate([own, tile[group_points : group_points + 8]], axis=0)
                at = (here, slice(None), slice((2 * g + t) * 128, (2 * g + t + 1) * 128))
                acc_ref[at] = jnp.where(fresh, own, acc_ref[at] + own)

    @pl.when(used == 0)
    def _():
        acc_ref[0] = jnp.zeros(acc_ref.shape[1:], F32)

    alone = last == 0
    column = lax.broadcasted_iota(jnp.int32, (128, 128), 1)
    tail = jnp.where(alone, -1, lab[0] + last).astype(F32)
    send_ref[:, 512:640] = jnp.where(column == 0, lab[0].astype(F32), tail)
    for t in range(4):
        cut = slice(t * 128, (t + 1) * 128)
        at = slice(t * dh, (t + 1) * dh)
        head = acc_ref[0, :, cut]
        foot = acc_ref[last, :, cut]
        foot = jnp.where(alone, jnp.zeros_like(foot), foot)
        send_ref[at, 0:128] = head[:dh]
        send_ref[at, 128:256] = foot[:dh]
        send_ref[at, 256:384] = jnp.broadcast_to(head[dh : dh + 1], (dh, 128))
        send_ref[at, 384:512] = jnp.broadcast_to(foot[dh : dh + 1], (dh, 128))


def owner_kernel(r_ref, o_ref):
    labels = r_ref[:, 512:640]
    rows = jnp.concatenate([labels[:, 0:1], labels[:, 1:2]], axis=0)
    rows = jnp.broadcast_to(rows, (256, 256))
    same = (rows == rows.T).astype(F32)
    data = jnp.concatenate(
        [
            jnp.concatenate([r_ref[:, 0:128], r_ref[:, 256:384]], axis=1),
            jnp.concatenate([r_ref[:, 128:256], r_ref[:, 384:512]], axis=1),
        ],
        axis=0,
    )
    whole = _dot(same, data, ((1,), (0,)), HIGHEST)
    tokens = whole[:, :128] / (whole[:, 128:] + 1.0)
    o_ref[:, 0:128] = tokens[:128]
    o_ref[:, 128:256] = tokens[128:]


def spread_kernel(
    tal, start, slot, meta, x_ref, w_ref, acc_ref, tok_ref, maps_ref, out_proj_ref,
    o_hbm,
    o_ref, mix_ref, sems,
):
    blocks, block, width = o_hbm.shape
    dh = maps_ref.shape[1]
    heads = width // dh
    group = heads // 2
    parts = w_ref.shape[1] // heads
    rows = group * parts
    count = meta[1]
    used = meta[2]
    last = meta[3]
    pieces = blocks // PIECE
    spare = mix_ref.shape[0] - 1

    def copy(i):
        part = pl.ds(i * PIECE, PIECE)
        return pltpu.make_async_copy(o_ref.at[part], o_hbm.at[part], sems.at[i])

    def attend(ats):
        row = lax.broadcasted_iota(jnp.int32, (128, 128), 0) // parts
        col = lax.broadcasted_iota(jnp.int32, (128, 128), 1) // parts
        lane = lax.broadcasted_iota(jnp.int32, (dh, 128), 1)
        maps = jnp.concatenate([maps_ref[i].T for i in range(3)], axis=0)
        projected = []
        for at in ats:
            tokens = []
            for t in range(4):
                kept = acc_ref[at, :, t * 128 : (t + 1) * 128]
                token = kept[:dh] / (kept[dh : dh + 1] + 1.0)
                token = jnp.where(at == last, tok_ref[t * dh : (t + 1) * dh, 128:256], token)
                tokens.append(jnp.where(at == 0, tok_ref[t * dh : (t + 1) * dh, 0:128], token))
            projected.append(_dot3(maps, jnp.concatenate(tokens, axis=1)))
        tiles = [(n, t) for n in range(len(ats)) for t in range(4)]
        scores = []
        for n, t in tiles:
            q, k = (projected[n][i * dh : (i + 1) * dh, t * 128 : (t + 1) * 128] for i in range(2))
            kh, kl = _split(k * (dh**-0.5 * LOG2E), 2)
            qh, ql = _split(q, 2)
            left = jnp.concatenate([kh, kl, kh], axis=0)
            scores.append(_dot(left, jnp.concatenate([qh, qh, ql], axis=0), ((0,), (0,))))
        probs = []
        for score in scores:
            score = jnp.where(row == col, score, -1e38)
            e = jnp.exp2(score - jnp.max(score, axis=0, keepdims=True))
            probs.append(e / jnp.sum(e, axis=0, keepdims=True))
        mixes = [
            _dot3(projected[n][2 * dh :, t * 128 : (t + 1) * 128], prob)
            for (n, t), prob in zip(tiles, probs)
        ]
        for (n, t), mixed in zip(tiles, mixes):
            for s in range(2):
                own = jnp.where(lane // parts == s, mixed, 0.0).astype(BF16)
                r = ((2 * t + s) % group) * dh
                c = (t % 2) * 128
                mix_ref[ats[n], t // 2, r : r + dh, c : c + 128] = own
                mix_ref[ats[n], t // 2, r : r + dh, 128 - c : 256 - c] = jnp.zeros_like(own)

    def blend(n):
        s = start[n]
        return jnp.concatenate(
            [
                _dot(
                    mix_ref[slot[n], g],
                    jnp.concatenate([w_ref[s + b, g * rows : (g + 1) * rows] for b in range(UNIT)], axis=1),
                    ((1,), (0,)),
                )
                for g in range(2)
            ],
            axis=0,
        ).astype(BF16)

    def finish(n, mixed):
        s = start[n]
        point = lax.broadcasted_iota(jnp.int32, (block, width), 0)
        projected = _dot(mixed, out_proj_ref[...], ((0,), (0,)))
        for b in range(UNIT):
            whole = x_ref[s + b].astype(F32) + projected[b * block : (b + 1) * block]
            live = point < tal[jnp.minimum(s + b, blocks - 1)]
            o_ref[s + b] = jnp.where(live, whole, 0.0).astype(BF16)

    @pl.loop(used // PIECE * PIECE, blocks)
    def _(b):
        o_ref[b] = jnp.zeros((block, width), BF16)

    idle = (used + PIECE - 1) // PIECE

    @pl.when(used > 0)
    def _():
        @pl.loop(0, (last + 2) // 2)
        def _(j):
            attend([2 * j, jnp.where(2 * j + 1 > last, spare, 2 * j + 1)])

    def step(j, sent):
        units = [BATCH * j + n for n in range(BATCH)]
        mixed = [blend(n) for n in units]
        for n, m in zip(units, mixed):
            finish(n, m)
        final = start[jnp.minimum(BATCH * (j + 1), count)]
        final = jnp.where(final == used, idle, final // PIECE)

        @pl.loop(sent, final)
        def _(i):
            copy(i).start()

        return final

    lax.fori_loop(0, (count + BATCH - 1) // BATCH, step, jnp.int32(0))

    @pl.loop(idle, pieces)
    def _(i):
        copy(i).start()

    for i in range(pieces):
        copy(i).wait()


def on_device(
    vertex_values,
    position_domain_label,
    position_vertex_tally,
    normalizer_gain,
    embedding_matrix,
    partition_input_matrix,
    partition_score_matrix,
    softmax_sharpness,
    partition_attention_maps,
    readout_matrix,
):
    slots, block, width = vertex_values.shape
    heads = softmax_sharpness.shape[0]
    dh, parts = partition_score_matrix.shape
    points = UNIT * block
    pieces = slots // PIECE
    room = slots + UNIT
    local = slots // 2 + 2
    smem = pl.BlockSpec(memory_space=pltpu.SMEM)
    vmem = pl.BlockSpec(memory_space=pltpu.VMEM)
    hbm = pl.BlockSpec(memory_space=pltpu.HBM)
    params = pltpu.CompilerParams(vmem_limit_bytes=24 << 20)
    far = lambda a: pltpu.with_memory_space_constraint(a, pltpu.HBM)
    x, shares, sums, send, start, slot, meta = pl.pallas_call(
        gather_kernel,
        name="gather",
        in_specs=[hbm] * 8,
        out_specs=[vmem, vmem, vmem, vmem, smem, smem, smem],
        out_shape=[
            pltpu.VMEM((room, block, width), BF16),
            pltpu.VMEM((room, heads * parts, block), BF16),
            pltpu.VMEM((local, dh + 8, heads * parts), F32),
            jax.ShapeDtypeStruct((128, 640), F32),
            jax.ShapeDtypeStruct((2 * slots,), jnp.int32),
            jax.ShapeDtypeStruct((2 * slots,), jnp.int32),
            jax.ShapeDtypeStruct((8,), jnp.int32),
        ],
        scratch_shapes=[
            pltpu.SMEM((slots,), jnp.int32),
            pltpu.SMEM((slots,), jnp.int32),
            pltpu.SMEM((heads,), F32),
            pltpu.VMEM((1, width), F32),
            pltpu.VMEM((width, width), BF16),
            pltpu.VMEM((width, width), BF16),
            pltpu.VMEM((dh, parts), BF16),
            pltpu.VMEM((2 * width, width), BF16),
            pltpu.VMEM((heads, parts, 3 * dh), BF16),
            pltpu.VMEM((width, width), BF16),
            pltpu.VMEM((room, width, block), BF16),
            pltpu.SemaphoreType.DMA((pieces,)),
            pltpu.SemaphoreType.DMA((7,)),
        ],
        compiler_params=params,
    )(
        far(position_domain_label),
        far(position_vertex_tally),
        far(softmax_sharpness),
        far(vertex_values),
        far(normalizer_gain.reshape(1, width)),
        far(embedding_matrix),
        far(partition_input_matrix),
        far(partition_score_matrix),
    )
    got = lax.all_to_all(send, AXES, 0, 0, tiled=True)
    back = pl.pallas_call(
        owner_kernel,
        name="owner",
        out_shape=jax.ShapeDtypeStruct((128, 256), F32),
        compiler_params=params,
    )(got)
    tokens = lax.all_to_all(back, AXES, 0, 0, tiled=True)
    keep = lambda a: pltpu.with_memory_space_constraint(a, pltpu.VMEM)
    return pl.pallas_call(
        spread_kernel,
        name="spread",
        in_specs=[smem, smem, smem, smem, vmem, vmem, vmem, vmem, vmem, vmem],
        out_specs=hbm,
        out_shape=jax.ShapeDtypeStruct(vertex_values.shape, BF16),
        scratch_shapes=[
            pltpu.VMEM((room, block, width), BF16),
            pltpu.VMEM((local, 2, width // 2, heads * parts // 2), BF16),
            pltpu.SemaphoreType.DMA((pieces,)),
        ],
        compiler_params=params,
    )(
        position_vertex_tally,
        start,
        slot,
        meta,
        keep(x),
        keep(shares),
        keep(sums),
        tokens,
        partition_attention_maps,
        readout_matrix,
    )


def solution(mesh):
    rows = P(AXES)
    return jax.shard_map(
        on_device,
        mesh=mesh,
        in_specs=(P(AXES, None, None), rows, rows, P(), P(), P(), P(), P(), P(), P()),
        out_specs=P(AXES, None, None),
        check_vma=False,
    )
```

```python
import jax
import jax.numpy as jnp
from jax import lax
from jax.experimental import pallas as pl
from jax.experimental.pallas import tpu as pltpu
from jax.sharding import PartitionSpec as P

MESHES = 64
UNIT = 4
PIECE = 4
BATCH = 4
WIDE = 8
LOG2E = 1.4426950408889634
AXES = ("grp", "dev")
F32 = jnp.float32
BF16 = jnp.bfloat16
HIGHEST = lax.Precision.HIGHEST


def _dot(a, b, dims, precision=None):
    return lax.dot_general(a, b, (dims, ((), ())), precision=precision, preferred_element_type=F32)


def _split(a, terms):
    out = []
    for _ in range(terms):
        out.append(a.astype(BF16))
        a = a - out[-1].astype(F32)
    return out


def _dot3(a, b):
    ah, al = _split(a, 2)
    bh, bl = _split(b, 2)
    return _dot(
        jnp.concatenate([ah, al, ah], axis=1), jnp.concatenate([bh, bh, bl], axis=0), ((1,), (0,))
    )


def _units(lab, start, slot, blocks):
    count = jnp.int32(0)
    begin = jnp.int32(0)
    used = jnp.int32(0)
    for b in range(blocks):
        mesh = lab[b]
        in_use = mesh < MESHES
        opens = b - begin == UNIT
        opens = jnp.logical_or(opens, mesh != lab[b - 1]) if b else jnp.bool_(True)
        opens = jnp.logical_and(opens, in_use)
        start[count] = b
        slot[count] = mesh - lab[0]
        begin = jnp.where(opens, b, begin)
        count = count + opens.astype(jnp.int32)
        used = used + in_use.astype(jnp.int32)
    return count, used


def gather_kernel(
    lab_hbm, tal_hbm, sharp_hbm, x_hbm, gain_hbm, emb_hbm, pin_hbm, score_hbm,
    x_ref, w_ref, acc_ref, send_ref, start, slot, meta,
    lab, tal, sharp, gain_ref, emb_ref, pin_ref, score_ref, wt_ref, st_ref, mean_ref, f_ref, sems, param_sems,
):
    blocks, block, width = x_hbm.shape
    points = UNIT * block
    heads = sharp.shape[0]
    dh = width // heads
    parts = score_ref.shape[1]
    group = heads // 2
    spare = acc_ref.shape[0] - 1
    pieces = blocks // PIECE

    def copy(i):
        part = pl.ds(i * PIECE, PIECE)
        return pltpu.make_async_copy(x_hbm.at[part], x_ref.at[part], sems.at[i])

    given = (
        (lab_hbm, lab),
        (tal_hbm, tal),
        (sharp_hbm, sharp),
        (gain_hbm, gain_ref),
        (emb_hbm, emb_ref),
        (pin_hbm, pin_ref),
        (score_hbm, score_ref),
    )
    params = [pltpu.make_async_copy(a, b, param_sems.at[n]) for n, (a, b) in enumerate(given)]
    for p in params:
        p.start()
    for i in range(pieces):
        copy(i).start()
    row = lax.broadcasted_iota(jnp.int32, (width, width), 0)
    col = lax.broadcasted_iota(jnp.int32, (width, width), 1)
    mean_ref[...] = ((row == col).astype(F32) - 1.0 / width).astype(BF16)
    for p in params[:3]:
        p.wait()
    count, used = _units(lab, start, slot, blocks)
    start[count] = used
    for n in range(BATCH):
        start[count + 1 + n] = blocks
        slot[count + n] = spare
    meta[0] = lab[0]
    meta[1] = count
    meta[2] = used
    last = jnp.where(used > 0, slot[jnp.maximum(count - 1, 0)], 0)
    meta[3] = last
    for p in params[3:]:
        p.wait()
    gain_ref[...] = gain_ref[...] * width**0.5
    wt_ref[:width, :] = emb_ref[...].astype(F32).T.astype(BF16)
    wt_ref[width:, :] = pin_ref[...].astype(F32).T.astype(BF16)
    score = score_ref[...].astype(F32).T
    for h in range(heads):
        factor = jnp.full(score.shape, LOG2E, F32) / jnp.full(score.shape, sharp[h], F32)
        st_ref[h] = jnp.concatenate(_split(score * factor, 3), axis=1)

    group_points = group * dh
    ones = jnp.ones((16, block), BF16)
    lane = lax.broadcasted_iota(jnp.int32, (dh, 128), 1)

    def normalize(s):
        x = x_ref[pl.ds(s, UNIT)].reshape(points, width)
        centre = _dot(x, mean_ref[...], ((1,), (0,)))
        return centre

    def scale(centre):
        square = jnp.sum(centre * centre, axis=1, keepdims=True)
        return (centre * lax.rsqrt(square + 1e-05 * width) * gain_ref[...]).astype(BF16)

    def weigh(logit, live):
        e = jnp.exp2(logit - jnp.max(logit, axis=0, keepdims=True))
        return (e * (live / jnp.sum(e, axis=0, keepdims=True))).astype(BF16)

    def living(s):
        spot = lax.broadcasted_iota(jnp.int32, (1, points), 1)
        limit = jnp.zeros((1, points), jnp.int32)
        for b in range(UNIT):
            limit = jnp.where(spot // block == b, b * block + tal[s + b], limit)
        return (spot < limit).astype(F32)

    def put(ref, s, row, value):
        for b in range(UNIT):
            ref[s + b, row : row + value.shape[0], :] = value[:, b * block : (b + 1) * block]

    stride = WIDE * UNIT
    trips = (used + stride - 1) // stride

    @pl.loop(0, trips)
    def _(j):
        for i in range(stride // PIECE):
            copy(j * (stride // PIECE) + i).wait()
        first = [j * stride + n * UNIT for n in range(WIDE)]
        centres, normed, both = {}, {}, {}

        def project(pair):
            def embed(n):
                both[n] = _dot(wt_ref[...], normed.pop(n), ((1,), (1,))).astype(BF16)
                put(f_ref, first[n], 0, both[n][:width])

            steps = [lambda n=n: centres.__setitem__(n, normalize(first[n])) for n in pair]
            steps += [lambda n=n: normed.__setitem__(n, scale(centres.pop(n))) for n in pair]
            return steps + [lambda n=n: embed(n) for n in pair]

        pairs = [(n, n + 1) for n in range(0, WIDE, 2)]
        for step in project(pairs[0]):
            step()
        for at, pair in enumerate(pairs):
            coming = project(pairs[at + 1]) if at + 1 < len(pairs) else []
            lives = {n: living(first[n]) for n in pair}
            items = [(h, n) for h in range(heads) for n in pair]
            due = [int(0.8 * k * (len(items) + 2) / max(1, len(coming))) for k in range(len(coming))]
            ahead = {}
            for k in range(len(items) + 2):
                if k < len(items):
                    h, n = items[k]
                    mid = both[n][width + h * dh : width + (h + 1) * dh, :]
                    ahead[h, n] = _dot(st_ref[h], jnp.concatenate([mid, mid, mid], axis=0), ((1,), (0,)))
                for step, when in zip(coming, due):
                    if when == k:
                        step()
                if k >= 2:
                    h, n = items[k - 2]
                    put(w_ref, first[n], h * parts, weigh(ahead.pop((h, n)), lives[n]))

    @pl.loop(trips * (stride // PIECE), pieces)
    def _(i):
        copy(i).wait()

    for b in range(UNIT):
        w_ref[trips * stride + b] = jnp.zeros(w_ref.shape[1:], BF16)

    def product(n, g):
        s = start[n]
        rows = slice(g * group * parts, (g + 1) * group * parts)
        total = None
        for b in range(UNIT):
            part = jnp.concatenate([f_ref[s + b, g * group_points : (g + 1) * group_points], ones], axis=0)
            part = jnp.where(s + b < start[n + 1], part, jnp.zeros_like(part))
            one = _dot(part, w_ref[s + b, rows], ((1,), (1,)))
            total = one if total is None else total + one
        return total

    @pl.loop(0, (count + BATCH - 1) // BATCH)
    def _(j):
        units = [j * BATCH + n for n in range(BATCH)]
        totals = [(n, g, product(n, g)) for n in units for g in range(2)]
        for n, g, total in totals:
            here = slot[n]
            fresh = jnp.logical_or(n == 0, slot[jnp.maximum(n - 1, 0)] != here)
            for t in range(2):
                tile = total[:, t * 128 : (t + 1) * 128]
                r = 2 * t * dh
                own = jnp.where(lane < parts, tile[r : r + dh], tile[r + dh : r + 2 * dh])
                own = jnp.concatenate([own, tile[group_points : group_points + 8]], axis=0)
                at = (here, slice(None), slice((2 * g + t) * 128, (2 * g + t + 1) * 128))
                acc_ref[at] = jnp.where(fresh, own, acc_ref[at] + own)

    @pl.when(used == 0)
    def _():
        acc_ref[0] = jnp.zeros(acc_ref.shape[1:], F32)

    alone = last == 0
    column = lax.broadcasted_iota(jnp.int32, (128, 128), 1)
    tail = jnp.where(alone, -1, lab[0] + last).astype(F32)
    send_ref[:, 512:640] = jnp.where(column == 0, lab[0].astype(F32), tail)
    for t in range(4):
        cut = slice(t * 128, (t + 1) * 128)
        at = slice(t * dh, (t + 1) * dh)
        head = acc_ref[0, :, cut]
        foot = acc_ref[last, :, cut]
        foot = jnp.where(alone, jnp.zeros_like(foot), foot)
        send_ref[at, 0:128] = head[:dh]
        send_ref[at, 128:256] = foot[:dh]
        send_ref[at, 256:384] = jnp.broadcast_to(head[dh : dh + 1], (dh, 128))
        send_ref[at, 384:512] = jnp.broadcast_to(foot[dh : dh + 1], (dh, 128))


def owner_kernel(r_ref, o_ref):
    labels = r_ref[:, 512:640]
    rows = jnp.concatenate([labels[:, 0:1], labels[:, 1:2]], axis=0)
    rows = jnp.broadcast_to(rows, (256, 256))
    same = (rows == rows.T).astype(F32)
    data = jnp.concatenate(
        [
            jnp.concatenate([r_ref[:, 0:128], r_ref[:, 256:384]], axis=1),
            jnp.concatenate([r_ref[:, 128:256], r_ref[:, 384:512]], axis=1),
        ],
        axis=0,
    )
    whole = _dot(same, data, ((1,), (0,)), HIGHEST)
    tokens = whole[:, :128] / (whole[:, 128:] + 1.0)
    o_ref[:, 0:128] = tokens[:128]
    o_ref[:, 128:256] = tokens[128:]


def spread_kernel(
    tal, start, slot, meta, x_ref, w_ref, acc_ref, tok_ref, maps_ref, out_proj_ref,
    o_hbm,
    o_ref, mix_ref, sems,
):
    blocks, block, width = o_hbm.shape
    dh = maps_ref.shape[1]
    heads = width // dh
    group = heads // 2
    parts = w_ref.shape[1] // heads
    rows = group * parts
    count = meta[1]
    used = meta[2]
    last = meta[3]
    pieces = blocks // PIECE
    spare = mix_ref.shape[0] - 1

    def copy(i):
        part = pl.ds(i * PIECE, PIECE)
        return pltpu.make_async_copy(o_ref.at[part], o_hbm.at[part], sems.at[i])

    def attend(ats):
        row = lax.broadcasted_iota(jnp.int32, (128, 128), 0) // parts
        col = lax.broadcasted_iota(jnp.int32, (128, 128), 1) // parts
        lane = lax.broadcasted_iota(jnp.int32, (dh, 128), 1)
        maps = jnp.concatenate([maps_ref[i].T for i in range(3)], axis=0)
        projected = []
        for at in ats:
            tokens = []
            for t in range(4):
                kept = acc_ref[at, :, t * 128 : (t + 1) * 128]
                token = kept[:dh] / (kept[dh : dh + 1] + 1.0)
                token = jnp.where(at == last, tok_ref[t * dh : (t + 1) * dh, 128:256], token)
                tokens.append(jnp.where(at == 0, tok_ref[t * dh : (t + 1) * dh, 0:128], token))
            projected.append(_dot3(maps, jnp.concatenate(tokens, axis=1)))
        tiles = [(n, t) for n in range(len(ats)) for t in range(4)]
        scores = []
        for n, t in tiles:
            q, k = (projected[n][i * dh : (i + 1) * dh, t * 128 : (t + 1) * 128] for i in range(2))
            kh, kl = _split(k * (dh**-0.5 * LOG2E), 2)
            qh, ql = _split(q, 2)
            left = jnp.concatenate([kh, kl, kh], axis=0)
            scores.append(_dot(left, jnp.concatenate([qh, qh, ql], axis=0), ((0,), (0,))))
        probs = []
        for score in scores:
            score = jnp.where(row == col, score, -1e38)
            e = jnp.exp2(score - jnp.max(score, axis=0, keepdims=True))
            probs.append(e / jnp.sum(e, axis=0, keepdims=True))
        mixes = [
            _dot3(projected[n][2 * dh :, t * 128 : (t + 1) * 128], prob)
            for (n, t), prob in zip(tiles, probs)
        ]
        for (n, t), mixed in zip(tiles, mixes):
            for s in range(2):
                own = jnp.where(lane // parts == s, mixed, 0.0).astype(BF16)
                r = ((2 * t + s) % group) * dh
                c = (t % 2) * 128
                mix_ref[ats[n], t // 2, r : r + dh, c : c + 128] = own
                mix_ref[ats[n], t // 2, r : r + dh, 128 - c : 256 - c] = jnp.zeros_like(own)

    def blend(n):
        s = start[n]
        return jnp.concatenate(
            [
                _dot(
                    mix_ref[slot[n], g],
                    jnp.concatenate([w_ref[s + b, g * rows : (g + 1) * rows] for b in range(UNIT)], axis=1),
                    ((1,), (0,)),
                )
                for g in range(2)
            ],
            axis=0,
        ).astype(BF16)

    def finish(n, mixed):
        s = start[n]
        point = lax.broadcasted_iota(jnp.int32, (block, width), 0)
        projected = _dot(mixed, out_proj_ref[...], ((0,), (0,)))
        for b in range(UNIT):
            whole = x_ref[s + b].astype(F32) + projected[b * block : (b + 1) * block]
            live = point < tal[jnp.minimum(s + b, blocks - 1)]
            o_ref[s + b] = jnp.where(live, whole, 0.0).astype(BF16)

    @pl.loop(used // PIECE * PIECE, blocks)
    def _(b):
        o_ref[b] = jnp.zeros((block, width), BF16)

    idle = (used + PIECE - 1) // PIECE

    @pl.when(used > 0)
    def _():
        @pl.loop(0, (last + 2) // 2)
        def _(j):
            attend([2 * j, jnp.where(2 * j + 1 > last, spare, 2 * j + 1)])

    def step(j, sent):
        units = [BATCH * j + n for n in range(BATCH)]
        mixed = [blend(n) for n in units]
        for n, m in zip(units, mixed):
            finish(n, m)
        final = start[jnp.minimum(BATCH * (j + 1), count)]
        final = jnp.where(final == used, idle, final // PIECE)

        @pl.loop(sent, final)
        def _(i):
            copy(i).start()

        return final

    lax.fori_loop(0, (count + BATCH - 1) // BATCH, step, jnp.int32(0))

    @pl.loop(idle, pieces)
    def _(i):
        copy(i).start()

    for i in range(pieces):
        copy(i).wait()


def on_device(
    vertex_values,
    position_domain_label,
    position_vertex_tally,
    normalizer_gain,
    embedding_matrix,
    partition_input_matrix,
    partition_score_matrix,
    softmax_sharpness,
    partition_attention_maps,
    readout_matrix,
):
    slots, block, width = vertex_values.shape
    heads = softmax_sharpness.shape[0]
    dh, parts = partition_score_matrix.shape
    points = UNIT * block
    pieces = slots // PIECE
    room = slots + UNIT
    local = slots // 2 + 2
    smem = pl.BlockSpec(memory_space=pltpu.SMEM)
    vmem = pl.BlockSpec(memory_space=pltpu.VMEM)
    hbm = pl.BlockSpec(memory_space=pltpu.HBM)
    params = pltpu.CompilerParams(vmem_limit_bytes=24 << 20)
    far = lambda a: pltpu.with_memory_space_constraint(a, pltpu.HBM)
    x, shares, sums, send, start, slot, meta = pl.pallas_call(
        gather_kernel,
        name="gather",
        in_specs=[hbm] * 8,
        out_specs=[vmem, vmem, vmem, vmem, smem, smem, smem],
        out_shape=[
            pltpu.VMEM((room, block, width), BF16),
            pltpu.VMEM((room, heads * parts, block), BF16),
            pltpu.VMEM((local, dh + 8, heads * parts), F32),
            jax.ShapeDtypeStruct((128, 640), F32),
            jax.ShapeDtypeStruct((2 * slots,), jnp.int32),
            jax.ShapeDtypeStruct((2 * slots,), jnp.int32),
            jax.ShapeDtypeStruct((8,), jnp.int32),
        ],
        scratch_shapes=[
            pltpu.SMEM((slots,), jnp.int32),
            pltpu.SMEM((slots,), jnp.int32),
            pltpu.SMEM((heads,), F32),
            pltpu.VMEM((1, width), F32),
            pltpu.VMEM((width, width), BF16),
            pltpu.VMEM((width, width), BF16),
            pltpu.VMEM((dh, parts), BF16),
            pltpu.VMEM((2 * width, width), BF16),
            pltpu.VMEM((heads, parts, 3 * dh), BF16),
            pltpu.VMEM((width, width), BF16),
            pltpu.VMEM((room, width, block), BF16),
            pltpu.SemaphoreType.DMA((pieces,)),
            pltpu.SemaphoreType.DMA((7,)),
        ],
        compiler_params=params,
    )(
        far(position_domain_label),
        far(position_vertex_tally),
        far(softmax_sharpness),
        far(vertex_values),
        far(normalizer_gain.reshape(1, width)),
        far(embedding_matrix),
        far(partition_input_matrix),
        far(partition_score_matrix),
    )
    got = lax.all_to_all(send, AXES, 0, 0, tiled=True)
    back = pl.pallas_call(
        owner_kernel,
        name="owner",
        out_shape=jax.ShapeDtypeStruct((128, 256), F32),
        compiler_params=params,
    )(got)
    tokens = lax.all_to_all(back, AXES, 0, 0, tiled=True)
    keep = lambda a: pltpu.with_memory_space_constraint(a, pltpu.VMEM)
    return pl.pallas_call(
        spread_kernel,
        name="spread",
        in_specs=[smem, smem, smem, smem, vmem, vmem, vmem, vmem, vmem, vmem],
        out_specs=hbm,
        out_shape=jax.ShapeDtypeStruct(vertex_values.shape, BF16),
        scratch_shapes=[
            pltpu.VMEM((room, block, width), BF16),
            pltpu.VMEM((local, 2, width // 2, heads * parts // 2), BF16),
            pltpu.SemaphoreType.DMA((pieces,)),
        ],
        compiler_params=params,
    )(
        position_vertex_tally,
        start,
        slot,
        meta,
        keep(x),
        keep(shares),
        keep(sums),
        tokens,
        partition_attention_maps,
        readout_matrix,
    )


def solution(mesh):
    rows = P(AXES)
    return jax.shard_map(
        on_device,
        mesh=mesh,
        in_specs=(P(AXES, None, None), rows, rows, P(), P(), P(), P(), P(), P(), P()),
        out_specs=P(AXES, None, None),
        check_vma=False,
    )
```
